32 devices in a mesh: blk: 2 (over x), tp: 4 (over z), qg: 4 (over y, core).
Axes of the slice: x: 2, y: 2, z: 4, core: 2. Of those that a mesh axis runs over, the one named last changes fastest.
Arguments:
- hidden_states: bfloat16 [1536, 4096], P(('blk', 'tp'), 'qg'), may hold values from -8 to 8
- query_states: bfloat16 [256, 4096], P('tp', 'qg'), may hold values from -8 to 8
- w_query: bfloat16 [4096, 4096], P('qg', 'tp'), may hold values from -0.25 to 0.25
- w_key: bfloat16 [4096, 1024], P('qg', 'tp'), may hold values from -0.09375 to 0.09375
- w_value: bfloat16 [4096, 1024], P('qg', 'tp'), may hold values from -0.09375 to 0.09375
- slot_order: int32 [4], replicated, may hold values from 0 to 3, each once
Outputs:
- attention: bfloat16 [1536, 4096], P(('blk', 'qg'), 'tp')
- decoded: bfloat16 [256, 4096], P('qg', 'tp')
The draws below stay inside these ranges and needn't reach their ends.
Inputs may be any that keep to these rules, and one draw needn't show every extreme that they name: slot_order holds every number of 0 to 3 once.
All inputs are finite; a program needn't handle non-finite values.
Results may differ from the reference program's by a relative error of at most 0.00775.
The reference program's roundings to bfloat16 on the way count: a program that leaves them out, or rounds other values in their place, can miss the bound.
Values may be sent and summed in bfloat16 or wider, within the bound.
A program may use at most 128 MiB of HBM per device.

```python
import math
import jax
import jax.numpy as jnp
from jax import lax

D = 4096
HEADS = 32
KV_HEADS = 8
HEAD_DIM = 128
QUERIES = 256
SEQ = 1536
SPAN = 384
SLOTS = 4


def draw_rows(key, row_count, columns, period):
    base_key, pick_key, forced_key, sign_key, size_key = jax.random.split(key, 5)
    drawn = jax.random.normal(base_key, (row_count, columns), jnp.float32)
    return jnp.clip(drawn, -8.0, 8.0).astype(jnp.bfloat16)


def draw_hidden_states(key, part):
    return draw_rows(jax.random.fold_in(key, 11), SEQ, D, 256)


def draw_query_states(key, part):
    return draw_rows(jax.random.fold_in(key, 23), QUERIES, D, 16)


def shard_levels(stream_key, extent, cuts, low, largest):
    def one(axis_at, blocks):
        heights = jax.random.uniform(jax.random.fold_in(jax.random.fold_in(stream_key, 6), axis_at), (blocks,), jnp.float32, low / len(cuts), largest / len(cuts))
        return jnp.repeat(jnp.exp(heights), extent[axis_at] // blocks).reshape((-1,) + (1,) * (len(extent) - axis_at - 1))

    gain = one(*cuts[0])
    for cut in cuts[1:]:
        gain = gain * one(*cut)
    return gain


def normal_values(own_key, shape, spread, most, pieces=(), kind=jnp.bfloat16):
    result = spread * jax.random.normal(own_key, shape, jnp.float32)
    if pieces:
        result = result * shard_levels(own_key, shape, pieces, -0.22, 0.18)
    return jnp.clip(result, -most, most).astype(kind)


def setup_inputs(seed: int = 0) -> dict:
    splits = jax.random.split(jax.random.key(seed), 7)
    hidden_states = draw_hidden_states(jax.random.fold_in(splits[6], 71), 0)
    query_states = draw_query_states(jax.random.fold_in(splits[6], 71), 0)
    w_query = normal_values(splits[2], (D, HEADS * HEAD_DIM), (D // 9) ** -0.5, 0.25, ((0, 4), (1, 4)))
    w_key = normal_values(splits[3], (D, KV_HEADS * HEAD_DIM), D ** -0.5, 0.09375, ((0, 4), (1, 4)))
    w_value = normal_values(splits[4], (D, KV_HEADS * HEAD_DIM), D ** -0.5, 0.09375, ((0, 4), (1, 4)))
    slot_order = jax.random.permutation(splits[5], SLOTS).astype(jnp.int32)
    return {"hidden_states": hidden_states, "query_states": query_states, "w_query": w_query, "w_key": w_key, "w_value": w_value, "slot_order": slot_order}


rope_base = 500000.0

def rotate(value_heads, position):
    full_dim = value_heads.shape[-1]
    half_dim = full_dim // 2
    frequency = jnp.float32(rope_base) ** (jnp.arange(half_dim, dtype=jnp.float32) * jnp.float32(-2.0 / full_dim))
    angles = position[:, None] * frequency[None, :]
    cosine = jnp.cos(angles)[:, None, :]
    sine_table = jnp.sin(angles)[:, None, :]
    front_half = value_heads[..., :half_dim]
    back_half = value_heads[..., half_dim:]
    return jnp.concatenate([front_half * cosine - back_half * sine_table, back_half * cosine + front_half * sine_table], axis=-1)

def attend(queries, key_heads, value_heads, query_pos, key_pos):
    scaling = 1.0 / math.sqrt(queries.shape[-1])
    scores = jnp.einsum('rgad,kgd->grak', queries.astype(jnp.float32), key_heads) * scaling
    if query_pos is not None:
        allowed = key_pos[None, None, None, :] <= query_pos[None, :, None, None]
        scores = jnp.where(allowed, scores, -jnp.inf)
    running_max = lax.optimization_barrier(jnp.max(scores, axis=-1, keepdims=True))
    weights = jnp.exp(scores - running_max)
    normalizer = lax.optimization_barrier(jnp.sum(weights, axis=-1))
    rounded = lax.optimization_barrier(weights.astype(jnp.bfloat16)).astype(jnp.float32)
    weighted = jnp.einsum('grak,kgd->rgad', rounded, value_heads)
    return (weighted / jnp.transpose(normalizer, (1, 0, 2))[..., None]).astype(jnp.bfloat16)

def reference(hidden_states, query_states, w_query, w_key, w_value, slot_order):
    sharing = HEADS // KV_HEADS
    row_ids = jnp.arange(SEQ, dtype=jnp.int32)
    positions = (slot_order[row_ids // SPAN] * SPAN + row_ids % SPAN).astype(jnp.int32)
    pos_float = positions.astype(jnp.float32)
    query_sum = jnp.dot(hidden_states, w_query, preferred_element_type=jnp.float32)
    queries = rotate(query_sum.reshape(SEQ, HEADS, HEAD_DIM), pos_float).astype(jnp.bfloat16)
    key_sum = jnp.dot(hidden_states, w_key, preferred_element_type=jnp.float32)
    key_heads = rotate(key_sum.reshape(SEQ, KV_HEADS, HEAD_DIM), pos_float).astype(jnp.bfloat16)
    value_heads = jnp.dot(hidden_states, w_value, preferred_element_type=jnp.float32).astype(jnp.bfloat16)
    keys_wide = key_heads.astype(jnp.float32)
    values_wide = value_heads.reshape(SEQ, KV_HEADS, HEAD_DIM).astype(jnp.float32)
    block_size = math.gcd(SEQ, 128)
    grouped = queries.reshape(SEQ // block_size, block_size, KV_HEADS, sharing, HEAD_DIM)
    spans = positions.reshape(SEQ // block_size, block_size)

    def one_block(paired):
        return attend(paired[0], keys_wide, values_wide, paired[1], positions)
    attention = lax.map(one_block, (grouped, spans)).reshape(SEQ, HEADS * HEAD_DIM)
    fresh_pos = jnp.full((QUERIES,), SEQ, jnp.float32)
    decode_sum = jnp.dot(query_states, w_query, preferred_element_type=jnp.float32)
    decode_query = rotate(decode_sum.reshape(QUERIES, HEADS, HEAD_DIM), fresh_pos).astype(jnp.bfloat16)
    decode_query = decode_query.reshape(QUERIES, KV_HEADS, sharing, HEAD_DIM)
    decoded = attend(decode_query, keys_wide, values_wide, None, None).reshape(QUERIES, HEADS * HEAD_DIM)
    return (attention, decoded)
```

```python
import functools
import math

import jax
import jax.numpy as jnp
import numpy as np
from jax import lax
from jax.experimental import pallas as pl
from jax.experimental.pallas import tpu as pltpu
from jax.sharding import PartitionSpec as P

HEAD_DIM = 128
ROPE_BASE = 500000.0
FLOOR = -1e30
TILE = 256
MESH = pl.DeviceIdType.MESH


def swap_halves(v):
    return pltpu.roll(v, HEAD_DIM // 2, 1)


def kernel(
    dims,
    slot,
    freq,
    hid,
    dec,
    wq_in,
    wk_in,
    wv_in,
    att_out,
    dec_out,
    own,
    xbuf,
    wq,
    wkv,
    qpart,
    qrecv,
    kvpart,
    kvrecv,
    kvall,
    qfin,
    sbuf,
    lsem,
    osem,
    xs,
    xr,
    ws,
    wr,
    qs,
    qr,
    ks_sem,
    kr_sem,
    cs_sem,
    cr_sem,
):
    nb, nz, nq, span = dims
    b = lax.axis_index("blk")
    z = lax.axis_index("tp")
    q = lax.axis_index("qg")
    c = lax.rem(q, 2)
    y = q // 2
    sib = (b, z, q + 1 - 2 * c)
    yp = (b, z, lax.rem(q + 2, nq))
    rows = hid.shape[0]
    drows = dec.shape[0]
    all_rows = rows + drows
    kvc = wk_in.shape[1]
    nt = wq_in.shape[1] // TILE
    heads = wq_in.shape[1] // HEAD_DIM
    kvh = kvc // HEAD_DIM
    sharing = heads // kvh
    group = rows * nz
    seq = group * nb
    kz = z // 2
    is_handler = lax.rem(z, 2) == c

    def local_x(dst):
        return (
            pltpu.make_async_copy(hid, dst.at[pl.ds(0, rows)], lsem.at[0]),
            pltpu.make_async_copy(dec, dst.at[pl.ds(rows, drows)], lsem.at[1]),
        )

    @pl.when(is_handler)
    def _():
        for cp in local_x(xbuf.at[kz, c]):
            cp.start()

    @pl.when(jnp.logical_not(is_handler))
    def _():
        for cp in local_x(own):
            cp.start()

    wlocal = (
        pltpu.make_async_copy(wq_in, wq.at[c], lsem.at[2]),
        pltpu.make_async_copy(wk_in, wkv.at[c, :, pl.ds(0, kvc)], lsem.at[3]),
        pltpu.make_async_copy(wv_in, wkv.at[c, :, pl.ds(kvc, kvc)], lsem.at[4]),
    )
    for cp in wlocal:
        cp.start()

    bar = pltpu.get_barrier_semaphore()

    def greet(dev):
        pl.semaphore_signal(bar, inc=1, device_id=dev, device_id_type=MESH)

    greet(sib)
    greet(yp)
    for o in range(1, nb):
        ob = lax.rem(b + o, nb)
        greet((ob, z, q))
        greet((ob, z, q + 1 - 2 * c))

    @pl.when(z > 0)
    def _():
        greet((b, z - 1, q))

    @pl.when(z < nz - 1)
    def _():
        greet((b, z + 1, q))

    @pl.when(jnp.logical_or(z == 0, z == nz - 1))
    def _():
        pl.semaphore_wait(bar, 2 + 2 * (nb - 1) + 1)

    @pl.when(jnp.logical_and(z > 0, z < nz - 1))
    def _():
        pl.semaphore_wait(bar, 2 + 2 * (nb - 1) + 2)

    def remote(src, dst, ss, rs, dev):
        return pltpu.make_async_remote_copy(
            src_ref=src, dst_ref=dst, send_sem=ss, recv_sem=rs, device_id=dev, device_id_type=MESH
        )

    own_send = remote(own, xbuf.at[kz, c], osem, xr.at[kz, c], sib)

    @pl.when(is_handler)
    def _():
        for cp in local_x(xbuf.at[kz, c]):
            cp.wait()

    @pl.when(jnp.logical_not(is_handler))
    def _():
        for cp in local_x(own):
            cp.wait()
        own_send.start()

    wremote = (
        remote(wk_in, wkv.at[c, :, pl.ds(0, kvc)], ws.at[1], wr.at[1], sib),
        remote(wv_in, wkv.at[c, :, pl.ds(kvc, kvc)], ws.at[2], wr.at[2], sib),
        remote(wq_in, wq.at[c], ws.at[0], wr.at[0], sib),
    )

    def relay(k, h, act):
        s = 2 * k + c
        ref = xbuf.at[k, h]

        @pl.when(jnp.logical_and(z <= s, z > 0))
        def _():
            act(remote(ref, ref, xs.at[k, h, 0], xr.at[k, h], (b, z - 1, q)))

        @pl.when(jnp.logical_and(z >= s, z < nz - 1))
        def _():
            act(remote(ref, ref, xs.at[k, h, 1], xr.at[k, h], (b, z + 1, q)))

    def landed(k, h):
        ref = xbuf.at[k, h]
        remote(ref, ref, xs.at[k, h, 0], xr.at[k, h], sib).wait_recv()

    def arrive(k):
        @pl.when(2 * k + c != z)
        def _():
            landed(k, c)

        relay(k, c, lambda cp: cp.start())
        landed(k, 1 - c)
        relay(k, 1 - c, lambda cp: cp.start())

    def kv_exchange(k):
        return remote(kvpart.at[k], kvrecv.at[k], ks_sem.at[k], kr_sem.at[k], yp)

    def q_exchange(k, t):
        return remote(qpart.at[k, t], qrecv.at[t], qs.at[t], qr.at[t], yp)

    def project(k):
        for t in range(2 * kvc // TILE):
            cols = pl.ds(t * TILE, TILE)
            kvpart[k, :, cols] = jnp.dot(
                xbuf[k, 0, :rows], wkv[0, :, cols], preferred_element_type=jnp.float32
            ) + jnp.dot(xbuf[k, 1, :rows], wkv[1, :, cols], preferred_element_type=jnp.float32)
        kv_exchange(k).start()

        def one(t, carry):
            cols = pl.ds(pl.multiple_of(t * TILE, TILE), TILE)
            qpart[k, t] = jnp.dot(
                xbuf[k, 0], wq[0, :, cols], preferred_element_type=jnp.float32
            ) + jnp.dot(xbuf[k, 1], wq[1, :, cols], preferred_element_type=jnp.float32)

            @pl.when(k != y)
            def _():
                q_exchange(k, t).start()

            return carry

        lax.fori_loop(0, nt, one, 0)

    lane = lax.broadcasted_iota(jnp.int32, (1, HEAD_DIM), 1)
    sign = jnp.where(lane < HEAD_DIM // 2, -1.0, 1.0).astype(jnp.float32)

    def block_pos(s):
        start = b * group + s * rows
        return slot[start // span] * span + lax.rem(start, span)

    def tables(pos):
        angles = pos.astype(jnp.float32) * freq[...]
        return jnp.cos(angles), jnp.sin(angles) * sign

    def cache_sends(k):
        s = 2 * k + c
        ref = kvall.at[b, s]
        devs = []
        for o in range(1, nb):
            ob = lax.rem(b + o, nb)
            devs += [(ob, z, q), (ob, z, q + 1 - 2 * c)]
        devs.append(sib)
        return [
            remote(ref, ref, cs_sem.at[k, i], cr_sem.at[b, s], dev) for i, dev in enumerate(devs)
        ]

    def finish_kv(k):
        s = 2 * k + c
        kv_exchange(k).wait_recv()
        total = kvpart[k] + kvrecv[k]
        pos = block_pos(s) + lax.broadcasted_iota(jnp.int32, (rows, 1), 0)
        cosine, sine = tables(pos)
        for g in range(kvh):
            v = total[:, g * HEAD_DIM : (g + 1) * HEAD_DIM]
            kvall[b, s, :, g * HEAD_DIM : (g + 1) * HEAD_DIM] = (
                v * cosine + swap_halves(v) * sine
            ).astype(jnp.bfloat16)
        kvall[b, s, :, kvc:] = total[:, kvc:].astype(jnp.bfloat16)
        for cp in cache_sends(k):
            cp.start()

    first = kz
    second = 1 - kz
    near = jnp.abs(z - 2 * first - c)
    far = jnp.abs(z - 2 * second - c)
    tie = near == far

    @pl.when(is_handler)
    def _():
        relay(kz, c, lambda cp: cp.start())

    for cp in wremote:
        cp.start()

    @pl.when(jnp.logical_not(is_handler))
    def _():
        landed(first, c)
        relay(first, c, lambda cp: cp.start())

    landed(first, 1 - c)
    relay(first, 1 - c, lambda cp: cp.start())

    @pl.when(tie)
    def _():
        arrive(second)

    for cp in wlocal:
        cp.wait()
    other = (
        remote(wk_in, wkv.at[1 - c, :, pl.ds(0, kvc)], ws.at[1], wr.at[1], sib),
        remote(wv_in, wkv.at[1 - c, :, pl.ds(kvc, kvc)], ws.at[2], wr.at[2], sib),
        remote(wq_in, wq.at[1 - c], ws.at[0], wr.at[0], sib),
    )
    for cp in other:
        cp.wait_recv()
    project(first)

    @pl.when(jnp.logical_not(tie))
    def _():
        arrive(second)
        finish_kv(first)

    project(second)

    @pl.when(tie)
    def _():
        finish_kv(first)

    finish_kv(second)

    row_id = lax.broadcasted_iota(jnp.int32, (all_rows, 1), 0)
    qpos = jnp.where(row_id < rows, block_pos(q) + row_id, seq)
    cosine, sine = tables(qpos)
    for t in range(nt):
        q_exchange(y, t).wait_recv()
        total = qpart[y, t] + qrecv[t]
        for h in range(TILE // HEAD_DIM):
            v = total[:, h * HEAD_DIM : (h + 1) * HEAD_DIM]
            qfin[t * (TILE // HEAD_DIM) + h] = (v * cosine + swap_halves(v) * sine).astype(
                jnp.bfloat16
            )

    for o in range(nb):
        ob = lax.rem(b + o, nb)
        for s in range(nz):
            ref = kvall.at[ob, s]
            wait = remote(ref, ref, cs_sem.at[0, 0], cr_sem.at[ob, s], sib).wait_recv
            if o == 0:
                pl.when(c != s % 2)(wait)
            else:
                wait()

    factor = math.log2(math.e) / math.sqrt(HEAD_DIM)
    unroll = nb <= 4

    def head(h, carry):
        qh = qfin[h]
        g = h // sharing
        kcols = pl.ds(pl.multiple_of(g * HEAD_DIM, HEAD_DIM), HEAD_DIM)
        vcols = pl.ds(pl.multiple_of(kvc + g * HEAD_DIM, HEAD_DIM), HEAD_DIM)

        def scores(j, m):
            keys = kvall[j, :, :, kcols].reshape(group, HEAD_DIM)
            s = lax.dot_general(
                qh, keys, (((1,), (1,)), ((), ())), preferred_element_type=jnp.float32
            )
            col = lax.broadcasted_iota(jnp.int32, (1, group), 1)
            kpos = jnp.zeros((1, group), jnp.int32)
            for i in range(group // span):
                inside = jnp.logical_and(col >= i * span, col < (i + 1) * span)
                kpos = jnp.where(
                    inside, slot[j * (group // span) + i] * span + col - i * span, kpos
                )
            s = jnp.where(kpos <= qpos, s, FLOOR)
            sbuf[j] = s
            return jnp.maximum(m, jnp.max(s, axis=1, keepdims=True))

        m = lax.fori_loop(
            0, nb, scores, jnp.full((all_rows, 1), FLOOR, jnp.float32), unroll=unroll
        )

        def weigh(j, state):
            norm, acc = state
            p = jnp.exp2((sbuf[j] - m) * factor)
            values = kvall[j, :, :, vcols].reshape(group, HEAD_DIM)
            norm = norm + jnp.sum(p, axis=1, keepdims=True)
            acc = acc + jnp.dot(
                p.astype(jnp.bfloat16), values, preferred_element_type=jnp.float32
            )
            return norm, acc

        norm, acc = lax.fori_loop(
            0,
            nb,
            weigh,
            (jnp.zeros((all_rows, 1), jnp.float32), jnp.zeros((all_rows, HEAD_DIM), jnp.float32)),
            unroll=unroll,
        )
        res = (acc / norm).astype(jnp.bfloat16)
        ocols = pl.ds(pl.multiple_of(h * HEAD_DIM, HEAD_DIM), HEAD_DIM)
        att_out[:, ocols] = res[:rows]
        dec_out[:, ocols] = res[rows:]
        return carry

    lax.fori_loop(0, heads, head, 0)

    @pl.when(jnp.logical_not(is_handler))
    def _():
        own_send.wait_send()

    for cp in wremote:
        cp.wait_send()
    for k in range(2):
        for h in range(2):
            relay(k, h, lambda cp: cp.wait_send())
        kv_exchange(k).wait_send()
        for cp in cache_sends(k):
            cp.wait_send()
    for t in range(nt):
        q_exchange(1 - y, t).wait_send()


def body(nb, nz, nq, hidden_states, query_states, w_query, w_key, w_value, slot_order):
    rows, depth = hidden_states.shape
    drows = query_states.shape[0]
    all_rows = rows + drows
    kvc = w_key.shape[1]
    nt = w_query.shape[1] // TILE
    heads = w_query.shape[1] // HEAD_DIM
    group = rows * nz
    span = group * nb // slot_order.shape[0]
    assert nz == 4 and nq == 4 and group % span == 0 and span % rows == 0
    exponent = np.arange(HEAD_DIM // 2, dtype=np.float64) * (-2.0 / HEAD_DIM)
    freq = np.float32(ROPE_BASE**exponent)
    freq = jnp.asarray(np.concatenate([freq, freq])[None, :])
    bf, f32 = jnp.bfloat16, jnp.float32
    dma = pltpu.SemaphoreType.DMA
    vm = pl.BlockSpec(memory_space=pltpu.VMEM)
    anyspace = pl.BlockSpec(memory_space=pl.ANY)
    return pl.pallas_call(
        functools.partial(kernel, (nb, nz, nq, span)),
        out_shape=(
            jax.ShapeDtypeStruct((rows, w_query.shape[1]), bf),
            jax.ShapeDtypeStruct((drows, w_query.shape[1]), bf),
        ),
        in_specs=[pl.BlockSpec(memory_space=pltpu.SMEM), vm] + [anyspace] * 5,
        out_specs=(vm, vm),
        scratch_shapes=[
            pltpu.VMEM((all_rows, depth), bf),
            pltpu.VMEM((2, 2, all_rows, depth), bf),
            pltpu.VMEM((2, depth, w_query.shape[1]), bf),
            pltpu.VMEM((2, depth, 2 * kvc), bf),
            pltpu.VMEM((2, nt, all_rows, TILE), f32),
            pltpu.VMEM((nt, all_rows, TILE), f32),
            pltpu.VMEM((2, rows, 2 * kvc), f32),
            pltpu.VMEM((2, rows, 2 * kvc), f32),
            pltpu.VMEM((nb, nz, rows, 2 * kvc), bf),
            pltpu.VMEM((heads, all_rows, HEAD_DIM), bf),
            pltpu.VMEM((nb, all_rows, group), f32),
            dma((5,)),
            dma,
            dma((2, 2, 2)),
            dma((2, 2)),
            dma((3,)),
            dma((3,)),
            dma((nt,)),
            dma((nt,)),
            dma((2,)),
            dma((2,)),
            dma((2, 2 * nb)),
            dma((nb, nz)),
        ],
        compiler_params=pltpu.CompilerParams(
            collective_id=0, has_side_effects=True, vmem_limit_bytes=60 * 1024 * 1024
        ),
    )(slot_order, freq, hidden_states, query_states, w_query, w_key, w_value)


def solution(mesh):
    sizes = (mesh.shape["blk"], mesh.shape["tp"], mesh.shape["qg"])
    return jax.shard_map(
        functools.partial(body, *sizes),
        mesh=mesh,
        in_specs=(
            P(("blk", "tp"), "qg"),
            P("tp", "qg"),
            P("qg", "tp"),
            P("qg", "tp"),
            P("qg", "tp"),
            P(),
        ),
        out_specs=(P(("blk", "qg"), "tp"), P("qg", "tp")),
        check_vma=False,
    )
```

```python
import functools
import math

import jax
import jax.numpy as jnp
import numpy as np
from jax import lax
from jax.experimental import pallas as pl
from jax.experimental.pallas import tpu as pltpu
from jax.sharding import PartitionSpec as P

HEAD_DIM = 128
ROPE_BASE = 500000.0
FLOOR = -1e30
TILE = 256
MESH = pl.DeviceIdType.MESH


def swap_halves(v):
    return pltpu.roll(v, HEAD_DIM // 2, 1)


def kernel(
    dims,
    slot,
    freq,
    hid,
    dec,
    wq_in,
    wk_in,
    wv_in,
    att_out,
    dec_out,
    own,
    xbuf,
    wq,
    wkv,
    qpart,
    qrecv,
    kvpart,
    kvrecv,
    kvall,
    sbuf,
    lsem,
    osem,
    xs,
    xr,
    ws,
    wr,
    qs,
    qr,
    ks_sem,
    kr_sem,
    cs_sem,
    cr_sem,
):
    nb, nz, nq, span = dims
    b = lax.axis_index("blk")
    z = lax.axis_index("tp")
    q = lax.axis_index("qg")
    c = lax.rem(q, 2)
    y = q // 2
    sib = (b, z, q + 1 - 2 * c)
    yp = (b, z, lax.rem(q + 2, nq))
    rows = hid.shape[0]
    drows = dec.shape[0]
    all_rows = rows + drows
    kvc = wk_in.shape[1]
    nt = wq_in.shape[1] // TILE
    kvh = kvc // HEAD_DIM
    sharing = wq_in.shape[1] // kvc
    group = rows * nz
    seq = group * nb
    kz = z // 2
    is_handler = lax.rem(z, 2) == c

    def local_x(dst):
        return (
            pltpu.make_async_copy(hid, dst.at[pl.ds(0, rows)], lsem.at[0]),
            pltpu.make_async_copy(dec, dst.at[pl.ds(rows, drows)], lsem.at[1]),
        )

    @pl.when(is_handler)
    def _():
        for cp in local_x(xbuf.at[kz, c]):
            cp.start()

    @pl.when(jnp.logical_not(is_handler))
    def _():
        for cp in local_x(own):
            cp.start()

    wlocal = (
        pltpu.make_async_copy(wq_in, wq.at[c], lsem.at[2]),
        pltpu.make_async_copy(wk_in, wkv.at[c, :, pl.ds(0, kvc)], lsem.at[3]),
        pltpu.make_async_copy(wv_in, wkv.at[c, :, pl.ds(kvc, kvc)], lsem.at[4]),
    )
    for cp in wlocal:
        cp.start()

    bar = pltpu.get_barrier_semaphore()

    def greet(dev):
        pl.semaphore_signal(bar, inc=1, device_id=dev, device_id_type=MESH)

    greet(sib)
    greet(yp)
    for o in range(1, nb):
        ob = lax.rem(b + o, nb)
        greet((ob, z, q))
        greet((ob, z, q + 1 - 2 * c))

    @pl.when(z > 0)
    def _():
        greet((b, z - 1, q))

    @pl.when(z < nz - 1)
    def _():
        greet((b, z + 1, q))

    @pl.when(jnp.logical_or(z == 0, z == nz - 1))
    def _():
        pl.semaphore_wait(bar, 2 + 2 * (nb - 1) + 1)

    @pl.when(jnp.logical_and(z > 0, z < nz - 1))
    def _():
        pl.semaphore_wait(bar, 2 + 2 * (nb - 1) + 2)

    def remote(src, dst, ss, rs, dev):
        return pltpu.make_async_remote_copy(
            src_ref=src, dst_ref=dst, send_sem=ss, recv_sem=rs, device_id=dev, device_id_type=MESH
        )

    own_send = remote(own, xbuf.at[kz, c], osem, xr.at[kz, c], sib)

    @pl.when(is_handler)
    def _():
        for cp in local_x(xbuf.at[kz, c]):
            cp.wait()

    @pl.when(jnp.logical_not(is_handler))
    def _():
        for cp in local_x(own):
            cp.wait()
        own_send.start()

    wremote = (
        remote(wk_in, wkv.at[c, :, pl.ds(0, kvc)], ws.at[1], wr.at[1], sib),
        remote(wv_in, wkv.at[c, :, pl.ds(kvc, kvc)], ws.at[2], wr.at[2], sib),
        remote(wq_in, wq.at[c], ws.at[0], wr.at[0], sib),
    )

    def relay(k, h, act):
        s = 2 * k + c
        ref = xbuf.at[k, h]

        @pl.when(jnp.logical_and(z <= s, z > 0))
        def _():
            act(remote(ref, ref, xs.at[k, h, 0], xr.at[k, h], (b, z - 1, q)))

        @pl.when(jnp.logical_and(z >= s, z < nz - 1))
        def _():
            act(remote(ref, ref, xs.at[k, h, 1], xr.at[k, h], (b, z + 1, q)))

    def landed(k, h):
        ref = xbuf.at[k, h]
        remote(ref, ref, xs.at[k, h, 0], xr.at[k, h], sib).wait_recv()

    def arrive(k):
        @pl.when(2 * k + c != z)
        def _():
            landed(k, c)

        relay(k, c, lambda cp: cp.start())
        landed(k, 1 - c)
        relay(k, 1 - c, lambda cp: cp.start())

    def kv_exchange(k):
        return remote(kvpart.at[k], kvrecv.at[k], ks_sem.at[k], kr_sem.at[k], yp)

    def q_exchange(k, t):
        return remote(qpart.at[k, t], qrecv.at[t], qs.at[t], qr.at[t], yp)

    def project(k):
        for t in range(2 * kvc // TILE):
            cols = pl.ds(t * TILE, TILE)
            kvpart[k, :, cols] = jnp.dot(
                xbuf[k, 0, :rows], wkv[0, :, cols], preferred_element_type=jnp.float32
            ) + jnp.dot(xbuf[k, 1, :rows], wkv[1, :, cols], preferred_element_type=jnp.float32)
        kv_exchange(k).start()

        def one(t, carry):
            cols = pl.ds(pl.multiple_of(t * TILE, TILE), TILE)
            qpart[k, t] = jnp.dot(
                xbuf[k, 0], wq[0, :, cols], preferred_element_type=jnp.float32
            ) + jnp.dot(xbuf[k, 1], wq[1, :, cols], preferred_element_type=jnp.float32)

            @pl.when(k != y)
            def _():
                q_exchange(k, t).start()

            return carry

        lax.fori_loop(0, nt, one, 0)

    lane = lax.broadcasted_iota(jnp.int32, (1, HEAD_DIM), 1)
    sign = jnp.where(lane < HEAD_DIM // 2, -1.0, 1.0).astype(jnp.float32)

    def block_pos(s):
        start = b * group + s * rows
        return slot[start // span] * span + lax.rem(start, span)

    def tables(pos):
        angles = pos.astype(jnp.float32) * freq[...]
        return jnp.cos(angles), jnp.sin(angles) * sign

    def cache_sends(k):
        s = 2 * k + c
        ref = kvall.at[b, s]
        devs = []
        for o in range(1, nb):
            ob = lax.rem(b + o, nb)
            devs += [(ob, z, q), (ob, z, q + 1 - 2 * c)]
        devs.append(sib)
        return [
            remote(ref, ref, cs_sem.at[k, i], cr_sem.at[b, s], dev) for i, dev in enumerate(devs)
        ]

    def finish_kv(k):
        s = 2 * k + c
        kv_exchange(k).wait_recv()
        total = kvpart[k] + kvrecv[k]
        pos = block_pos(s) + lax.broadcasted_iota(jnp.int32, (rows, 1), 0)
        cosine, sine = tables(pos)
        for g in range(kvh):
            v = total[:, g * HEAD_DIM : (g + 1) * HEAD_DIM]
            kvall[b, s, :, g * HEAD_DIM : (g + 1) * HEAD_DIM] = (
                v * cosine + swap_halves(v) * sine
            ).astype(jnp.bfloat16)
        kvall[b, s, :, kvc:] = total[:, kvc:].astype(jnp.bfloat16)
        for cp in cache_sends(k):
            cp.start()

    first = kz
    second = 1 - kz
    near = jnp.abs(z - 2 * first - c)
    far = jnp.abs(z - 2 * second - c)
    tie = near == far

    @pl.when(is_handler)
    def _():
        relay(kz, c, lambda cp: cp.start())

    for cp in wremote:
        cp.start()

    @pl.when(jnp.logical_not(is_handler))
    def _():
        landed(first, c)
        relay(first, c, lambda cp: cp.start())

    landed(first, 1 - c)
    relay(first, 1 - c, lambda cp: cp.start())

    @pl.when(tie)
    def _():
        arrive(second)

    for cp in wlocal:
        cp.wait()
    other = (
        remote(wk_in, wkv.at[1 - c, :, pl.ds(0, kvc)], ws.at[1], wr.at[1], sib),
        remote(wv_in, wkv.at[1 - c, :, pl.ds(kvc, kvc)], ws.at[2], wr.at[2], sib),
        remote(wq_in, wq.at[1 - c], ws.at[0], wr.at[0], sib),
    )
    for cp in other:
        cp.wait_recv()
    project(first)

    @pl.when(jnp.logical_not(tie))
    def _():
        arrive(second)
        finish_kv(first)

    project(second)

    @pl.when(tie)
    def _():
        finish_kv(first)

    finish_kv(second)

    row_id = lax.broadcasted_iota(jnp.int32, (all_rows, 1), 0)
    qpos = jnp.where(row_id < rows, block_pos(q) + row_id, seq)
    cosine, sine = tables(qpos)
    for o in range(nb):
        ob = lax.rem(b + o, nb)
        for s in range(nz):
            ref = kvall.at[ob, s]
            wait = remote(ref, ref, cs_sem.at[0, 0], cr_sem.at[ob, s], sib).wait_recv
            if o == 0:
                pl.when(c != s % 2)(wait)
            else:
                wait()

    factor = math.log2(math.e) / math.sqrt(HEAD_DIM)
    unroll = nb <= 4

    def head(h, qh, sbuf):
        g = h // sharing
        kcols = pl.ds(pl.multiple_of(g * HEAD_DIM, HEAD_DIM), HEAD_DIM)
        vcols = pl.ds(pl.multiple_of(kvc + g * HEAD_DIM, HEAD_DIM), HEAD_DIM)

        def scores(j, m):
            keys = kvall[j, :, :, kcols].reshape(group, HEAD_DIM)
            s = lax.dot_general(
                qh, keys, (((1,), (1,)), ((), ())), preferred_element_type=jnp.float32
            )
            col = lax.broadcasted_iota(jnp.int32, (1, group), 1)
            kpos = jnp.zeros((1, group), jnp.int32)
            for i in range(group // span):
                inside = jnp.logical_and(col >= i * span, col < (i + 1) * span)
                kpos = jnp.where(
                    inside, slot[j * (group // span) + i] * span + col - i * span, kpos
                )
            s = jnp.where(kpos <= qpos, s, FLOOR)
            sbuf[j] = s
            return jnp.maximum(m, jnp.max(s, axis=1, keepdims=True))

        m = lax.fori_loop(
            0, nb, scores, jnp.full((all_rows, 1), FLOOR, jnp.float32), unroll=unroll
        )

        def weigh(j, state):
            norm, acc = state
            p = jnp.exp2((sbuf[j] - m) * factor)
            values = kvall[j, :, :, vcols].reshape(group, HEAD_DIM)
            norm = norm + jnp.sum(p, axis=1, keepdims=True)
            acc = acc + jnp.dot(
                p.astype(jnp.bfloat16), values, preferred_element_type=jnp.float32
            )
            return norm, acc

        norm, acc = lax.fori_loop(
            0,
            nb,
            weigh,
            (jnp.zeros((all_rows, 1), jnp.float32), jnp.zeros((all_rows, HEAD_DIM), jnp.float32)),
            unroll=unroll,
        )
        res = (acc / norm).astype(jnp.bfloat16)
        ocols = pl.ds(pl.multiple_of(h * HEAD_DIM, HEAD_DIM), HEAD_DIM)
        att_out[:, ocols] = res[:rows]
        dec_out[:, ocols] = res[rows:]

    per = TILE // HEAD_DIM

    def tile_heads(t, carry):
        q_exchange(y, t).wait_recv()
        total = qpart[y, t] + qrecv[t]
        ready = []
        for i in range(per):
            v = total[:, i * HEAD_DIM : (i + 1) * HEAD_DIM]
            ready.append((v * cosine + swap_halves(v) * sine).astype(jnp.bfloat16))
        for i in range(per):
            head(t * per + i, ready[i], sbuf.at[i] if nb <= 4 else sbuf.at[0])
        return carry

    lax.fori_loop(0, nt, tile_heads, 0)

    @pl.when(jnp.logical_not(is_handler))
    def _():
        own_send.wait_send()

    for cp in wremote:
        cp.wait_send()
    for k in range(2):
        for h in range(2):
            relay(k, h, lambda cp: cp.wait_send())
        kv_exchange(k).wait_send()
        for cp in cache_sends(k):
            cp.wait_send()
    for t in range(nt):
        q_exchange(1 - y, t).wait_send()


def body(nb, nz, nq, hidden_states, query_states, w_query, w_key, w_value, slot_order):
    rows, depth = hidden_states.shape
    drows = query_states.shape[0]
    all_rows = rows + drows
    kvc = w_key.shape[1]
    nt = w_query.shape[1] // TILE
    group = rows * nz
    span = group * nb // slot_order.shape[0]
    assert nz == 4 and nq == 4 and group % span == 0 and span % rows == 0
    exponent = np.arange(HEAD_DIM // 2, dtype=np.float64) * (-2.0 / HEAD_DIM)
    freq = np.float32(ROPE_BASE**exponent)
    freq = jnp.asarray(np.concatenate([freq, freq])[None, :])
    bf, f32 = jnp.bfloat16, jnp.float32
    dma = pltpu.SemaphoreType.DMA
    vm = pl.BlockSpec(memory_space=pltpu.VMEM)
    anyspace = pl.BlockSpec(memory_space=pl.ANY)
    return pl.pallas_call(
        functools.partial(kernel, (nb, nz, nq, span)),
        out_shape=(
            jax.ShapeDtypeStruct((rows, w_query.shape[1]), bf),
            jax.ShapeDtypeStruct((drows, w_query.shape[1]), bf),
        ),
        in_specs=[pl.BlockSpec(memory_space=pltpu.SMEM), vm] + [anyspace] * 5,
        out_specs=(vm, vm),
        scratch_shapes=[
            pltpu.VMEM((all_rows, depth), bf),
            pltpu.VMEM((2, 2, all_rows, depth), bf),
            pltpu.VMEM((2, depth, w_query.shape[1]), bf),
            pltpu.VMEM((2, depth, 2 * kvc), bf),
            pltpu.VMEM((2, nt, all_rows, TILE), f32),
            pltpu.VMEM((nt, all_rows, TILE), f32),
            pltpu.VMEM((2, rows, 2 * kvc), f32),
            pltpu.VMEM((2, rows, 2 * kvc), f32),
            pltpu.VMEM((nb, nz, rows, 2 * kvc), bf),
            pltpu.VMEM((2 if nb <= 4 else 1, nb, all_rows, group), f32),
            dma((5,)),
            dma,
            dma((2, 2, 2)),
            dma((2, 2)),
            dma((3,)),
            dma((3,)),
            dma((nt,)),
            dma((nt,)),
            dma((2,)),
            dma((2,)),
            dma((2, 2 * nb)),
            dma((nb, nz)),
        ],
        compiler_params=pltpu.CompilerParams(
            collective_id=0, has_side_effects=True, vmem_limit_bytes=60 * 1024 * 1024
        ),
    )(slot_order, freq, hidden_states, query_states, w_query, w_key, w_value)


def solution(mesh):
    sizes = (mesh.shape["blk"], mesh.shape["tp"], mesh.shape["qg"])
    return jax.shard_map(
        functools.partial(body, *sizes),
        mesh=mesh,
        in_specs=(
            P(("blk", "tp"), "qg"),
            P("tp", "qg"),
            P("qg", "tp"),
            P("qg", "tp"),
            P("qg", "tp"),
            P(),
        ),
        out_specs=(P(("blk", "qg"), "tp"), P("qg", "tp")),
        check_vma=False,
    )
```

```python
import functools
import math

import jax
import jax.numpy as jnp
import numpy as np
from jax import lax
from jax.experimental import pallas as pl
from jax.experimental.pallas import tpu as pltpu
from jax.sharding import PartitionSpec as P

HEAD_DIM = 128
ROPE_BASE = 500000.0
FLOOR = -1e30
TILE = 256
MESH = pl.DeviceIdType.MESH


def swap_halves(v):
    return pltpu.roll(v, HEAD_DIM // 2, 1)


def kernel(
    dims,
    slot,
    freq,
    hid,
    dec,
    wq_in,
    wk_in,
    wv_in,
    att_out,
    dec_out,
    own,
    xbuf,
    wq,
    wkv,
    qpart,
    qrecv,
    kvpart,
    kvrecv,
    kvall,
    sbuf,
    lsem,
    osem,
    xs,
    xr,
    ws,
    wr,
    qs,
    qr,
    ks_sem,
    kr_sem,
    cs_sem,
    cr_sem,
    dbuf,
    ds_sem,
    dr_sem,
):
    nb, nz, nq, span = dims
    b = lax.axis_index("blk")
    z = lax.axis_index("tp")
    q = lax.axis_index("qg")
    c = lax.rem(q, 2)
    y = q // 2
    sib = (b, z, q + 1 - 2 * c)
    yp = (b, z, lax.rem(q + 2, nq))
    rows = hid.shape[0]
    split = dbuf.shape[0]
    drows = dec.shape[0] // split
    part = lax.rem(b, split)
    all_rows = rows + drows
    kvc = wk_in.shape[1]
    nt = wq_in.shape[1] // TILE
    kvh = kvc // HEAD_DIM
    sharing = wq_in.shape[1] // kvc
    group = rows * nz
    seq = group * nb
    kz = z // 2
    is_handler = lax.rem(z, 2) == c

    def local_x(dst):
        return (
            pltpu.make_async_copy(hid, dst.at[pl.ds(0, rows)], lsem.at[0]),
            pltpu.make_async_copy(
                dec.at[pl.ds(pl.multiple_of(part * drows, drows), drows)],
                dst.at[pl.ds(rows, drows)],
                lsem.at[1],
            ),
        )

    @pl.when(is_handler)
    def _():
        for cp in local_x(xbuf.at[kz, c]):
            cp.start()

    @pl.when(jnp.logical_not(is_handler))
    def _():
        for cp in local_x(own):
            cp.start()

    wlocal = (
        pltpu.make_async_copy(wq_in, wq.at[c], lsem.at[2]),
        pltpu.make_async_copy(wk_in, wkv.at[c, :, pl.ds(0, kvc)], lsem.at[3]),
        pltpu.make_async_copy(wv_in, wkv.at[c, :, pl.ds(kvc, kvc)], lsem.at[4]),
    )
    for cp in wlocal:
        cp.start()

    bar = pltpu.get_barrier_semaphore()

    def greet(dev):
        pl.semaphore_signal(bar, inc=1, device_id=dev, device_id_type=MESH)

    greet(sib)
    greet(yp)
    for o in range(1, nb):
        ob = lax.rem(b + o, nb)
        greet((ob, z, q))
        greet((ob, z, q + 1 - 2 * c))

    @pl.when(z > 0)
    def _():
        greet((b, z - 1, q))

    @pl.when(z < nz - 1)
    def _():
        greet((b, z + 1, q))

    @pl.when(jnp.logical_or(z == 0, z == nz - 1))
    def _():
        pl.semaphore_wait(bar, 2 + 2 * (nb - 1) + 1)

    @pl.when(jnp.logical_and(z > 0, z < nz - 1))
    def _():
        pl.semaphore_wait(bar, 2 + 2 * (nb - 1) + 2)

    def remote(src, dst, ss, rs, dev):
        return pltpu.make_async_remote_copy(
            src_ref=src, dst_ref=dst, send_sem=ss, recv_sem=rs, device_id=dev, device_id_type=MESH
        )

    own_send = remote(own, xbuf.at[kz, c], osem, xr.at[kz, c], sib)

    @pl.when(is_handler)
    def _():
        for cp in local_x(xbuf.at[kz, c]):
            cp.wait()

    @pl.when(jnp.logical_not(is_handler))
    def _():
        for cp in local_x(own):
            cp.wait()
        own_send.start()

    wremote = (
        remote(wk_in, wkv.at[c, :, pl.ds(0, kvc)], ws.at[1], wr.at[1], sib),
        remote(wv_in, wkv.at[c, :, pl.ds(kvc, kvc)], ws.at[2], wr.at[2], sib),
        remote(wq_in, wq.at[c], ws.at[0], wr.at[0], sib),
    )

    def relay(k, h, act):
        s = 2 * k + c
        ref = xbuf.at[k, h]

        @pl.when(jnp.logical_and(z <= s, z > 0))
        def _():
            act(remote(ref, ref, xs.at[k, h, 0], xr.at[k, h], (b, z - 1, q)))

        @pl.when(jnp.logical_and(z >= s, z < nz - 1))
        def _():
            act(remote(ref, ref, xs.at[k, h, 1], xr.at[k, h], (b, z + 1, q)))

    def landed(k, h):
        ref = xbuf.at[k, h]
        remote(ref, ref, xs.at[k, h, 0], xr.at[k, h], sib).wait_recv()

    def arrive(k):
        @pl.when(2 * k + c != z)
        def _():
            landed(k, c)

        relay(k, c, lambda cp: cp.start())
        landed(k, 1 - c)
        relay(k, 1 - c, lambda cp: cp.start())

    def kv_exchange(k):
        return remote(kvpart.at[k], kvrecv.at[k], ks_sem.at[k], kr_sem.at[k], yp)

    def q_exchange(k, t):
        return remote(qpart.at[k, t], qrecv.at[t], qs.at[t], qr.at[t], yp)

    def project(k):
        for t in range(2 * kvc // TILE):
            cols = pl.ds(t * TILE, TILE)
            kvpart[k, :, cols] = jnp.dot(
                xbuf[k, 0, :rows], wkv[0, :, cols], preferred_element_type=jnp.float32
            ) + jnp.dot(xbuf[k, 1, :rows], wkv[1, :, cols], preferred_element_type=jnp.float32)
        kv_exchange(k).start()

        def one(t, carry):
            cols = pl.ds(pl.multiple_of(t * TILE, TILE), TILE)
            qpart[k, t] = jnp.dot(
                xbuf[k, 0], wq[0, :, cols], preferred_element_type=jnp.float32
            ) + jnp.dot(xbuf[k, 1], wq[1, :, cols], preferred_element_type=jnp.float32)

            @pl.when(k != y)
            def _():
                q_exchange(k, t).start()

            return carry

        lax.fori_loop(0, nt, one, 0)

    lane = lax.broadcasted_iota(jnp.int32, (1, HEAD_DIM), 1)
    sign = jnp.where(lane < HEAD_DIM // 2, -1.0, 1.0).astype(jnp.float32)

    def block_pos(s):
        start = b * group + s * rows
        return slot[start // span] * span + lax.rem(start, span)

    def tables(pos):
        angles = pos.astype(jnp.float32) * freq[...]
        return jnp.cos(angles), jnp.sin(angles) * sign

    def cache_sends(k):
        s = 2 * k + c
        ref = kvall.at[b, s]
        devs = []
        for o in range(1, nb):
            ob = lax.rem(b + o, nb)
            devs += [(ob, z, q), (ob, z, q + 1 - 2 * c)]
        devs.append(sib)
        return [
            remote(ref, ref, cs_sem.at[k, i], cr_sem.at[b, s], dev) for i, dev in enumerate(devs)
        ]

    def finish_kv(k):
        s = 2 * k + c
        kv_exchange(k).wait_recv()
        total = kvpart[k] + kvrecv[k]
        pos = block_pos(s) + lax.broadcasted_iota(jnp.int32, (rows, 1), 0)
        cosine, sine = tables(pos)
        for g in range(kvh):
            v = total[:, g * HEAD_DIM : (g + 1) * HEAD_DIM]
            kvall[b, s, :, g * HEAD_DIM : (g + 1) * HEAD_DIM] = (
                v * cosine + swap_halves(v) * sine
            ).astype(jnp.bfloat16)
        kvall[b, s, :, kvc:] = total[:, kvc:].astype(jnp.bfloat16)
        for cp in cache_sends(k):
            cp.start()

    first = kz
    second = 1 - kz
    near = jnp.abs(z - 2 * first - c)
    far = jnp.abs(z - 2 * second - c)
    tie = near == far

    @pl.when(is_handler)
    def _():
        relay(kz, c, lambda cp: cp.start())

    for cp in wremote:
        cp.start()

    @pl.when(jnp.logical_not(is_handler))
    def _():
        landed(first, c)
        relay(first, c, lambda cp: cp.start())

    landed(first, 1 - c)
    relay(first, 1 - c, lambda cp: cp.start())

    @pl.when(tie)
    def _():
        arrive(second)

    for cp in wlocal:
        cp.wait()
    other = (
        remote(wk_in, wkv.at[1 - c, :, pl.ds(0, kvc)], ws.at[1], wr.at[1], sib),
        remote(wv_in, wkv.at[1 - c, :, pl.ds(kvc, kvc)], ws.at[2], wr.at[2], sib),
        remote(wq_in, wq.at[1 - c], ws.at[0], wr.at[0], sib),
    )
    for cp in other:
        cp.wait_recv()
    project(first)

    @pl.when(jnp.logical_not(tie))
    def _():
        arrive(second)
        finish_kv(first)

    project(second)

    @pl.when(tie)
    def _():
        finish_kv(first)

    finish_kv(second)

    row_id = lax.broadcasted_iota(jnp.int32, (all_rows, 1), 0)
    qpos = jnp.where(row_id < rows, block_pos(q) + row_id, seq)
    cosine, sine = tables(qpos)
    for o in range(nb):
        ob = lax.rem(b + o, nb)
        for s in range(nz):
            ref = kvall.at[ob, s]
            wait = remote(ref, ref, cs_sem.at[0, 0], cr_sem.at[ob, s], sib).wait_recv
            if o == 0:
                pl.when(c != s % 2)(wait)
            else:
                wait()

    factor = math.log2(math.e) / math.sqrt(HEAD_DIM)
    unroll = nb <= 4

    def decode_exchange(t):
        ref = dbuf.at[part, t]
        return remote(ref, ref, ds_sem.at[t], dr_sem.at[t], (b + 1 - 2 * part, z, q))

    def head(h, qh, sbuf):
        g = h // sharing
        kcols = pl.ds(pl.multiple_of(g * HEAD_DIM, HEAD_DIM), HEAD_DIM)
        vcols = pl.ds(pl.multiple_of(kvc + g * HEAD_DIM, HEAD_DIM), HEAD_DIM)

        def scores(j, m):
            keys = kvall[j, :, :, kcols].reshape(group, HEAD_DIM)
            s = lax.dot_general(
                qh, keys, (((1,), (1,)), ((), ())), preferred_element_type=jnp.float32
            )
            col = lax.broadcasted_iota(jnp.int32, (1, group), 1)
            kpos = jnp.zeros((1, group), jnp.int32)
            for i in range(group // span):
                inside = jnp.logical_and(col >= i * span, col < (i + 1) * span)
                kpos = jnp.where(
                    inside, slot[j * (group // span) + i] * span + col - i * span, kpos
                )
            s = jnp.where(kpos <= qpos, s, FLOOR)
            sbuf[j] = s
            return jnp.maximum(m, jnp.max(s, axis=1, keepdims=True))

        m = lax.fori_loop(
            0, nb, scores, jnp.full((all_rows, 1), FLOOR, jnp.float32), unroll=unroll
        )

        def weigh(j, state):
            norm, acc = state
            p = jnp.exp2((sbuf[j] - m) * factor)
            values = kvall[j, :, :, vcols].reshape(group, HEAD_DIM)
            norm = norm + jnp.sum(p, axis=1, keepdims=True)
            acc = acc + jnp.dot(
                p.astype(jnp.bfloat16), values, preferred_element_type=jnp.float32
            )
            return norm, acc

        norm, acc = lax.fori_loop(
            0,
            nb,
            weigh,
            (jnp.zeros((all_rows, 1), jnp.float32), jnp.zeros((all_rows, HEAD_DIM), jnp.float32)),
            unroll=unroll,
        )
        res = (acc / norm).astype(jnp.bfloat16)
        ocols = pl.ds(pl.multiple_of(h * HEAD_DIM, HEAD_DIM), HEAD_DIM)
        att_out[:, ocols] = res[:rows]
        return res[rows:]

    per = TILE // HEAD_DIM

    def tile_heads(t, carry):
        q_exchange(y, t).wait_recv()
        total = qpart[y, t] + qrecv[t]
        ready = []
        for i in range(per):
            v = total[:, i * HEAD_DIM : (i + 1) * HEAD_DIM]
            ready.append((v * cosine + swap_halves(v) * sine).astype(jnp.bfloat16))
        for i in range(per):
            res = head(t * per + i, ready[i], sbuf.at[i] if nb <= 4 else sbuf.at[0])
            dbuf[part, t, :, i * HEAD_DIM : (i + 1) * HEAD_DIM] = res
        if split == 2:
            decode_exchange(t).start()
        return carry

    lax.fori_loop(0, nt, tile_heads, 0)

    for t in range(nt):
        if split == 2:
            decode_exchange(t).wait_recv()
        for i in range(split):
            dec_out[i * drows : (i + 1) * drows, t * TILE : (t + 1) * TILE] = dbuf[i, t]

    if split == 2:
        for t in range(nt):
            decode_exchange(t).wait_send()

    @pl.when(jnp.logical_not(is_handler))
    def _():
        own_send.wait_send()

    for cp in wremote:
        cp.wait_send()
    for k in range(2):
        for h in range(2):
            relay(k, h, lambda cp: cp.wait_send())
        kv_exchange(k).wait_send()
        for cp in cache_sends(k):
            cp.wait_send()
    for t in range(nt):
        q_exchange(1 - y, t).wait_send()


def body(nb, nz, nq, hidden_states, query_states, w_query, w_key, w_value, slot_order):
    rows, depth = hidden_states.shape
    split = 2 if nb % 2 == 0 else 1
    drows = query_states.shape[0] // split
    all_rows = rows + drows
    kvc = w_key.shape[1]
    nt = w_query.shape[1] // TILE
    group = rows * nz
    span = group * nb // slot_order.shape[0]
    assert nz == 4 and nq == 4 and group % span == 0 and span % rows == 0
    exponent = np.arange(HEAD_DIM // 2, dtype=np.float64) * (-2.0 / HEAD_DIM)
    freq = np.float32(ROPE_BASE**exponent)
    freq = jnp.asarray(np.concatenate([freq, freq])[None, :])
    bf, f32 = jnp.bfloat16, jnp.float32
    dma = pltpu.SemaphoreType.DMA
    vm = pl.BlockSpec(memory_space=pltpu.VMEM)
    anyspace = pl.BlockSpec(memory_space=pl.ANY)
    return pl.pallas_call(
        functools.partial(kernel, (nb, nz, nq, span)),
        out_shape=(
            jax.ShapeDtypeStruct((rows, w_query.shape[1]), bf),
            jax.ShapeDtypeStruct((drows * split, w_query.shape[1]), bf),
        ),
        in_specs=[pl.BlockSpec(memory_space=pltpu.SMEM), vm] + [anyspace] * 5,
        out_specs=(vm, vm),
        scratch_shapes=[
            pltpu.VMEM((all_rows, depth), bf),
            pltpu.VMEM((2, 2, all_rows, depth), bf),
            pltpu.VMEM((2, depth, w_query.shape[1]), bf),
            pltpu.VMEM((2, depth, 2 * kvc), bf),
            pltpu.VMEM((2, nt, all_rows, TILE), f32),
            pltpu.VMEM((nt, all_rows, TILE), f32),
            pltpu.VMEM((2, rows, 2 * kvc), f32),
            pltpu.VMEM((2, rows, 2 * kvc), f32),
            pltpu.VMEM((nb, nz, rows, 2 * kvc), bf),
            pltpu.VMEM((2 if nb <= 4 else 1, nb, all_rows, group), f32),
            dma((5,)),
            dma,
            dma((2, 2, 2)),
            dma((2, 2)),
            dma((3,)),
            dma((3,)),
            dma((nt,)),
            dma((nt,)),
            dma((2,)),
            dma((2,)),
            dma((2, 2 * nb)),
            dma((nb, nz)),
            pltpu.VMEM((split, nt, drows, TILE), bf),
            dma((nt,)),
            dma((nt,)),
        ],
        compiler_params=pltpu.CompilerParams(
            collective_id=0, has_side_effects=True, vmem_limit_bytes=60 * 1024 * 1024
        ),
    )(slot_order, freq, hidden_states, query_states, w_query, w_key, w_value)


def solution(mesh):
    sizes = (mesh.shape["blk"], mesh.shape["tp"], mesh.shape["qg"])
    return jax.shard_map(
        functools.partial(body, *sizes),
        mesh=mesh,
        in_specs=(
            P(("blk", "tp"), "qg"),
            P("tp", "qg"),
            P("qg", "tp"),
            P("qg", "tp"),
            P("qg", "tp"),
            P(),
        ),
        out_specs=(P(("blk", "qg"), "tp"), P("qg", "tp")),
        check_vma=False,
    )
```

```python
import functools
import math

import jax
import jax.numpy as jnp
import numpy as np
from jax import lax
from jax.experimental import pallas as pl
from jax.experimental.pallas import tpu as pltpu
from jax.sharding import PartitionSpec as P

HEAD_DIM = 128
ROPE_BASE = 500000.0
FLOOR = -1e30
TILE = 256
MESH = pl.DeviceIdType.MESH


def swap_halves(v):
    return pltpu.roll(v, HEAD_DIM // 2, 1)


def kernel(
    dims,
    slot,
    freq,
    hid,
    dec,
    wq_in,
    wk_in,
    wv_in,
    att_out,
    dec_out,
    own,
    xbuf,
    wq,
    wkv,
    qpart,
    qrecv,
    kvpart,
    kvrecv,
    kvall,
    sbuf,
    lsem,
    osem,
    xs,
    xr,
    ws,
    wr,
    qs,
    qr,
    ks_sem,
    kr_sem,
    cs_sem,
    cr_sem,
    dbuf,
    ds_sem,
    dr_sem,
    vsend,
    vrecv,
    vs_sem,
    vr_sem,
):
    nb, nz, nq, span = dims
    b = lax.axis_index("blk")
    z = lax.axis_index("tp")
    q = lax.axis_index("qg")
    c = lax.rem(q, 2)
    y = q // 2
    sib = (b, z, q + 1 - 2 * c)
    yp = (b, z, lax.rem(q + 2, nq))
    rows = hid.shape[0]
    split = dbuf.shape[0]
    drows = dec.shape[0] // split
    part = lax.rem(b, split)
    all_rows = rows + drows
    kvc = wk_in.shape[1]
    nt = wq_in.shape[1] // TILE
    kvh = kvc // HEAD_DIM
    sharing = wq_in.shape[1] // kvc
    group = rows * nz
    seq = group * nb
    kz = z // 2
    is_handler = lax.rem(z, 2) == c

    def local_x(dst):
        return (
            pltpu.make_async_copy(hid, dst.at[pl.ds(0, rows)], lsem.at[0]),
            pltpu.make_async_copy(
                dec.at[pl.ds(pl.multiple_of(part * drows, drows), drows)],
                dst.at[pl.ds(rows, drows)],
                lsem.at[1],
            ),
        )

    @pl.when(is_handler)
    def _():
        for cp in local_x(xbuf.at[kz, c]):
            cp.start()

    @pl.when(jnp.logical_not(is_handler))
    def _():
        for cp in local_x(own):
            cp.start()

    wlocal = (
        pltpu.make_async_copy(wq_in, wq.at[c], lsem.at[2]),
        pltpu.make_async_copy(wk_in, wkv.at[c, :, pl.ds(0, kvc)], lsem.at[3]),
        pltpu.make_async_copy(wv_in, wkv.at[c, :, pl.ds(kvc, kvc)], lsem.at[4]),
    )
    for cp in wlocal:
        cp.start()

    bar = pltpu.get_barrier_semaphore()

    def greet(dev):
        pl.semaphore_signal(bar, inc=1, device_id=dev, device_id_type=MESH)

    greet(sib)
    greet(yp)
    for o in range(1, nb):
        ob = lax.rem(b + o, nb)
        greet((ob, z, q))
        greet((ob, z, q + 1 - 2 * c))

    @pl.when(z > 0)
    def _():
        greet((b, z - 1, q))

    @pl.when(z < nz - 1)
    def _():
        greet((b, z + 1, q))

    @pl.when(jnp.logical_or(z == 0, z == nz - 1))
    def _():
        pl.semaphore_wait(bar, 2 + 2 * (nb - 1) + 1)

    @pl.when(jnp.logical_and(z > 0, z < nz - 1))
    def _():
        pl.semaphore_wait(bar, 2 + 2 * (nb - 1) + 2)

    def remote(src, dst, ss, rs, dev):
        return pltpu.make_async_remote_copy(
            src_ref=src, dst_ref=dst, send_sem=ss, recv_sem=rs, device_id=dev, device_id_type=MESH
        )

    own_send = remote(own, xbuf.at[kz, c], osem, xr.at[kz, c], sib)

    @pl.when(is_handler)
    def _():
        for cp in local_x(xbuf.at[kz, c]):
            cp.wait()

    @pl.when(jnp.logical_not(is_handler))
    def _():
        for cp in local_x(own):
            cp.wait()
        own_send.start()

    wremote = (
        remote(wk_in, wkv.at[c, :, pl.ds(0, kvc)], ws.at[1], wr.at[1], sib),
        remote(wv_in, wkv.at[c, :, pl.ds(kvc, kvc)], ws.at[2], wr.at[2], sib),
        remote(wq_in, wq.at[c], ws.at[0], wr.at[0], sib),
    )

    def relay(k, h, act):
        s = 2 * k + c
        ref = xbuf.at[k, h]

        @pl.when(jnp.logical_and(z <= s, z > 0))
        def _():
            act(remote(ref, ref, xs.at[k, h, 0], xr.at[k, h], (b, z - 1, q)))

        @pl.when(jnp.logical_and(z >= s, z < nz - 1))
        def _():
            act(remote(ref, ref, xs.at[k, h, 1], xr.at[k, h], (b, z + 1, q)))

    def landed(k, h):
        ref = xbuf.at[k, h]
        remote(ref, ref, xs.at[k, h, 0], xr.at[k, h], sib).wait_recv()

    def arrive(k):
        @pl.when(2 * k + c != z)
        def _():
            landed(k, c)

        relay(k, c, lambda cp: cp.start())
        landed(k, 1 - c)
        relay(k, 1 - c, lambda cp: cp.start())

    def k_exchange(k):
        return remote(kvpart.at[k, 0], kvrecv.at[k], ks_sem.at[k], kr_sem.at[k], yp)

    def v_exchange(k):
        return remote(vsend.at[k], vrecv.at[k], vs_sem.at[k], vr_sem.at[k], yp)

    def q_exchange(k, t):
        return remote(qpart.at[k, t], qrecv.at[t], qs.at[t], qr.at[t], yp)

    def project(k):
        for t in range(2):
            cols = pl.ds(t * kvc, kvc)
            kvpart[k, t] = jnp.dot(
                xbuf[k, 0, :rows], wkv[0, :, cols], preferred_element_type=jnp.float32
            ) + jnp.dot(xbuf[k, 1, :rows], wkv[1, :, cols], preferred_element_type=jnp.float32)
            if t == 0:
                k_exchange(k).start()
            else:
                vsend[k] = kvpart[k, 1].astype(jnp.bfloat16)
                v_exchange(k).start()

        def one(t, carry):
            cols = pl.ds(pl.multiple_of(t * TILE, TILE), TILE)
            qpart[k, t] = jnp.dot(
                xbuf[k, 0], wq[0, :, cols], preferred_element_type=jnp.float32
            ) + jnp.dot(xbuf[k, 1], wq[1, :, cols], preferred_element_type=jnp.float32)

            @pl.when(k != y)
            def _():
                q_exchange(k, t).start()

            return carry

        lax.fori_loop(0, nt, one, 0)

    lane = lax.broadcasted_iota(jnp.int32, (1, HEAD_DIM), 1)
    sign = jnp.where(lane < HEAD_DIM // 2, -1.0, 1.0).astype(jnp.float32)

    def block_pos(s):
        start = b * group + s * rows
        return slot[start // span] * span + lax.rem(start, span)

    def tables(pos):
        angles = pos.astype(jnp.float32) * freq[...]
        return jnp.cos(angles), jnp.sin(angles) * sign

    def cache_sends(k):
        s = 2 * k + c
        ref = kvall.at[b, s]
        devs = []
        for o in range(1, nb):
            ob = lax.rem(b + o, nb)
            devs += [(ob, z, q), (ob, z, q + 1 - 2 * c)]
        devs.append(sib)
        return [
            remote(ref, ref, cs_sem.at[k, i], cr_sem.at[b, s], dev) for i, dev in enumerate(devs)
        ]

    def finish_kv(k):
        s = 2 * k + c
        pos = block_pos(s) + lax.broadcasted_iota(jnp.int32, (rows, 1), 0)
        cosine, sine = tables(pos)
        k_exchange(k).wait_recv()
        total = kvpart[k, 0] + kvrecv[k]
        for g in range(kvh):
            v = total[:, g * HEAD_DIM : (g + 1) * HEAD_DIM]
            kvall[b, s, :, g * HEAD_DIM : (g + 1) * HEAD_DIM] = (
                v * cosine + swap_halves(v) * sine
            ).astype(jnp.bfloat16)
        v_exchange(k).wait_recv()
        kvall[b, s, :, kvc:] = (kvpart[k, 1] + vrecv[k].astype(jnp.float32)).astype(jnp.bfloat16)
        for cp in cache_sends(k):
            cp.start()

    first = kz
    second = 1 - kz
    near = jnp.abs(z - 2 * first - c)
    far = jnp.abs(z - 2 * second - c)
    tie = near == far

    @pl.when(is_handler)
    def _():
        relay(kz, c, lambda cp: cp.start())

    for cp in wremote:
        cp.start()

    @pl.when(jnp.logical_not(is_handler))
    def _():
        landed(first, c)
        relay(first, c, lambda cp: cp.start())

    @pl.when(tie)
    def _():
        landed(second, c)
        relay(second, c, lambda cp: cp.start())

    landed(first, 1 - c)
    relay(first, 1 - c, lambda cp: cp.start())

    @pl.when(tie)
    def _():
        landed(second, 1 - c)
        relay(second, 1 - c, lambda cp: cp.start())

    for cp in wlocal:
        cp.wait()
    other = (
        remote(wk_in, wkv.at[1 - c, :, pl.ds(0, kvc)], ws.at[1], wr.at[1], sib),
        remote(wv_in, wkv.at[1 - c, :, pl.ds(kvc, kvc)], ws.at[2], wr.at[2], sib),
        remote(wq_in, wq.at[1 - c], ws.at[0], wr.at[0], sib),
    )
    for cp in other:
        cp.wait_recv()
    project(first)

    @pl.when(jnp.logical_not(tie))
    def _():
        arrive(second)
        finish_kv(first)

    project(second)

    @pl.when(tie)
    def _():
        finish_kv(first)

    finish_kv(second)

    row_id = lax.broadcasted_iota(jnp.int32, (all_rows, 1), 0)
    qpos = jnp.where(row_id < rows, block_pos(q) + row_id, seq)
    cosine, sine = tables(qpos)
    for o in range(nb):
        ob = lax.rem(b + o, nb)
        for s in range(nz):
            ref = kvall.at[ob, s]
            wait = remote(ref, ref, cs_sem.at[0, 0], cr_sem.at[ob, s], sib).wait_recv
            if o == 0:
                pl.when(c != s % 2)(wait)
            else:
                wait()

    factor = math.log2(math.e) / math.sqrt(HEAD_DIM)
    unroll = nb <= 4

    def decode_exchange(t):
        ref = dbuf.at[part, t]
        return remote(ref, ref, ds_sem.at[t], dr_sem.at[t], (b + 1 - 2 * part, z, q))

    def head(h, qh, sbuf):
        g = h // sharing
        kcols = pl.ds(pl.multiple_of(g * HEAD_DIM, HEAD_DIM), HEAD_DIM)
        vcols = pl.ds(pl.multiple_of(kvc + g * HEAD_DIM, HEAD_DIM), HEAD_DIM)

        def scores(j, m):
            keys = kvall[j, :, :, kcols].reshape(group, HEAD_DIM)
            s = lax.dot_general(
                qh, keys, (((1,), (1,)), ((), ())), preferred_element_type=jnp.float32
            )
            col = lax.broadcasted_iota(jnp.int32, (1, group), 1)
            kpos = jnp.zeros((1, group), jnp.int32)
            for i in range(group // span):
                inside = jnp.logical_and(col >= i * span, col < (i + 1) * span)
                kpos = jnp.where(
                    inside, slot[j * (group // span) + i] * span + col - i * span, kpos
                )
            s = jnp.where(kpos <= qpos, s, FLOOR)
            sbuf[j] = s
            return jnp.maximum(m, jnp.max(s, axis=1, keepdims=True))

        m = lax.fori_loop(
            0, nb, scores, jnp.full((all_rows, 1), FLOOR, jnp.float32), unroll=unroll
        )

        def weigh(j, state):
            norm, acc = state
            p = jnp.exp2((sbuf[j] - m) * factor)
            values = kvall[j, :, :, vcols].reshape(group, HEAD_DIM)
            norm = norm + jnp.sum(p, axis=1, keepdims=True)
            acc = acc + jnp.dot(
                p.astype(jnp.bfloat16), values, preferred_element_type=jnp.float32
            )
            return norm, acc

        norm, acc = lax.fori_loop(
            0,
            nb,
            weigh,
            (jnp.zeros((all_rows, 1), jnp.float32), jnp.zeros((all_rows, HEAD_DIM), jnp.float32)),
            unroll=unroll,
        )
        res = (acc / norm).astype(jnp.bfloat16)
        ocols = pl.ds(pl.multiple_of(h * HEAD_DIM, HEAD_DIM), HEAD_DIM)
        att_out[:, ocols] = res[:rows]
        return res[rows:]

    per = TILE // HEAD_DIM

    def tile_heads(t, carry):
        q_exchange(y, t).wait_recv()
        total = qpart[y, t] + qrecv[t]
        ready = []
        for i in range(per):
            v = total[:, i * HEAD_DIM : (i + 1) * HEAD_DIM]
            ready.append((v * cosine + swap_halves(v) * sine).astype(jnp.bfloat16))
        for i in range(per):
            res = head(t * per + i, ready[i], sbuf.at[i] if nb <= 4 else sbuf.at[0])
            dbuf[part, t, :, i * HEAD_DIM : (i + 1) * HEAD_DIM] = res
        if split == 2:
            decode_exchange(t).start()
        return carry

    lax.fori_loop(0, nt, tile_heads, 0)

    for t in range(nt):
        if split == 2:
            decode_exchange(t).wait_recv()
        for i in range(split):
            dec_out[i * drows : (i + 1) * drows, t * TILE : (t + 1) * TILE] = dbuf[i, t]

    if split == 2:
        for t in range(nt):
            decode_exchange(t).wait_send()

    @pl.when(jnp.logical_not(is_handler))
    def _():
        own_send.wait_send()

    for cp in wremote:
        cp.wait_send()
    for k in range(2):
        for h in range(2):
            relay(k, h, lambda cp: cp.wait_send())
        k_exchange(k).wait_send()
        v_exchange(k).wait_send()
        for cp in cache_sends(k):
            cp.wait_send()
    for t in range(nt):
        q_exchange(1 - y, t).wait_send()


def body(nb, nz, nq, hidden_states, query_states, w_query, w_key, w_value, slot_order):
    rows, depth = hidden_states.shape
    split = 2 if nb % 2 == 0 else 1
    drows = query_states.shape[0] // split
    all_rows = rows + drows
    kvc = w_key.shape[1]
    nt = w_query.shape[1] // TILE
    group = rows * nz
    span = group * nb // slot_order.shape[0]
    assert nz == 4 and nq == 4 and group % span == 0 and span % rows == 0
    exponent = np.arange(HEAD_DIM // 2, dtype=np.float64) * (-2.0 / HEAD_DIM)
    freq = np.float32(ROPE_BASE**exponent)
    freq = jnp.asarray(np.concatenate([freq, freq])[None, :])
    bf, f32 = jnp.bfloat16, jnp.float32
    dma = pltpu.SemaphoreType.DMA
    vm = pl.BlockSpec(memory_space=pltpu.VMEM)
    anyspace = pl.BlockSpec(memory_space=pl.ANY)
    return pl.pallas_call(
        functools.partial(kernel, (nb, nz, nq, span)),
        out_shape=(
            jax.ShapeDtypeStruct((rows, w_query.shape[1]), bf),
            jax.ShapeDtypeStruct((drows * split, w_query.shape[1]), bf),
        ),
        in_specs=[pl.BlockSpec(memory_space=pltpu.SMEM), vm] + [anyspace] * 5,
        out_specs=(vm, vm),
        scratch_shapes=[
            pltpu.VMEM((all_rows, depth), bf),
            pltpu.VMEM((2, 2, all_rows, depth), bf),
            pltpu.VMEM((2, depth, w_query.shape[1]), bf),
            pltpu.VMEM((2, depth, 2 * kvc), bf),
            pltpu.VMEM((2, nt, all_rows, TILE), f32),
            pltpu.VMEM((nt, all_rows, TILE), f32),
            pltpu.VMEM((2, 2, rows, kvc), f32),
            pltpu.VMEM((2, rows, kvc), f32),
            pltpu.VMEM((nb, nz, rows, 2 * kvc), bf),
            pltpu.VMEM((2 if nb <= 4 else 1, nb, all_rows, group), f32),
            dma((5,)),
            dma,
            dma((2, 2, 2)),
            dma((2, 2)),
            dma((3,)),
            dma((3,)),
            dma((nt,)),
            dma((nt,)),
            dma((2,)),
            dma((2,)),
            dma((2, 2 * nb)),
            dma((nb, nz)),
            pltpu.VMEM((split, nt, drows, TILE), bf),
            dma((nt,)),
            dma((nt,)),
            pltpu.VMEM((2, rows, kvc), bf),
            pltpu.VMEM((2, rows, kvc), bf),
            dma((2,)),
            dma((2,)),
        ],
        compiler_params=pltpu.CompilerParams(
            collective_id=0, has_side_effects=True, vmem_limit_bytes=60 * 1024 * 1024
        ),
    )(slot_order, freq, hidden_states, query_states, w_query, w_key, w_value)


def solution(mesh):
    sizes = (mesh.shape["blk"], mesh.shape["tp"], mesh.shape["qg"])
    return jax.shard_map(
        functools.partial(body, *sizes),
        mesh=mesh,
        in_specs=(
            P(("blk", "tp"), "qg"),
            P("tp", "qg"),
            P("qg", "tp"),
            P("qg", "tp"),
            P("qg", "tp"),
            P(),
        ),
        out_specs=(P(("blk", "qg"), "tp"), P("qg", "tp")),
        check_vma=False,
    )
```
